256 devices in a mesh: rep: 2 (over core), dp: 128 (over x, y, z).
Axes of the slice: x: 4, y: 4, z: 8, core: 2. Of those that a mesh axis runs over, the one named last changes fastest.
Arguments:
- g_w_gate: bfloat16 [256, 2, 896, 2304], P(('rep', 'dp')), parts along dimension 0
- g_w_up: bfloat16 [256, 2, 896, 2304], P(('rep', 'dp')), parts along dimension 0
- g_w_down: bfloat16 [256, 2, 2304, 896], P(('rep', 'dp')), parts along dimension 0
- w_gate: bfloat16 [2, 896, 2304], replicated
- w_up: bfloat16 [2, 896, 2304], replicated
- w_down: bfloat16 [2, 2304, 896], replicated
- m_w_gate: float32 [2, 896, 2304], P(None, 'dp')
- m_w_up: float32 [2, 896, 2304], P(None, 'dp')
- m_w_down: float32 [2, 2304, 896], P(None, 'dp')
- v_w_gate: float32 [2, 896, 2304], P(None, 'dp')
- v_w_up: float32 [2, 896, 2304], P(None, 'dp')
- v_w_down: float32 [2, 2304, 896], P(None, 'dp')
Outputs:
- output 1: bfloat16 [4, 896, 2304], P('rep'), parts along dimension 0
- output 2: bfloat16 [4, 896, 2304], P('rep'), parts along dimension 0
- output 3: bfloat16 [4, 2304, 896], P('rep'), parts along dimension 0
- output 4: float32 [4, 896, 2304], P('rep', 'dp'), parts along dimension 0
- output 5: float32 [4, 896, 2304], P('rep', 'dp'), parts along dimension 0
- output 6: float32 [4, 2304, 896], P('rep', 'dp'), parts along dimension 0
- output 7: float32 [4, 896, 2304], P('rep', 'dp'), parts along dimension 0
- output 8: float32 [4, 896, 2304], P('rep', 'dp'), parts along dimension 0
- output 9: float32 [4, 2304, 896], P('rep', 'dp'), parts along dimension 0
There are 2 independent parts. The reference program is written for one: setup_inputs(seed, part) draws one part's arguments, and reference() takes and returns one part's arrays. A program takes and returns all parts, laid end to end along the dimension named above; an argument that names none is the same for every part.
All inputs are finite; a program needn't handle non-finite values.
Results may differ from the reference program's by a relative error of at most 0.022.
Values are sent between devices in bfloat16 or wider.
A program may use at most 768 MiB of HBM per device.

```python
import jax
import jax.numpy as jnp
from jax import lax

DEVICES = 128
D = 896
FF = 2304
LAYERS = 2
NAMES = ("w_gate", "w_up", "w_down")
SHAPES = {"w_gate": (LAYERS, D, FF), "w_up": (LAYERS, D, FF), "w_down": (LAYERS, FF, D)}


def setup_inputs(seed: int = 0, part: int = 0) -> dict:
    kz, *keys = jax.random.split(jax.random.key(seed), 1 + 5 * len(NAMES))
    loud = 2.0 ** jax.random.uniform(kz, (), jnp.float32, -1.0, 1.0)
    drawn = {}
    for name, key, both in zip(NAMES, keys[:3], keys[3:6], strict=True):
        own = jax.random.normal(jax.random.fold_in(key, part), (DEVICES, *SHAPES[name]), jnp.float32)
        shared = jax.random.normal(jax.random.fold_in(both, part), SHAPES[name], jnp.float32)
        drawn["g_" + name] = (loud * (0.7 * shared / DEVICES + 0.7 * own * DEVICES**-0.5)).astype(jnp.bfloat16)
    for name, key in zip(NAMES, keys[6:9], strict=True):
        drawn[name] = (jax.random.normal(key, SHAPES[name], jnp.float32) * SHAPES[name][1] ** -0.5).astype(jnp.bfloat16)
    for name, key in zip(NAMES, keys[9:12], strict=True):
        drawn["m_" + name] = loud * 0.5 * jax.random.normal(key, SHAPES[name], jnp.float32)
    for name, key in zip(NAMES, keys[12:15], strict=True):
        drawn["v_" + name] = loud * loud * jax.random.uniform(key, SHAPES[name], jnp.float32, 0.5, 1.5)
    return drawn


def adamw(w, m, v, g):
    m = 0.9 * m + 0.1 * g
    v = 0.95 * v + 0.05 * g * g
    step = m * lax.rsqrt(v + 1e-8) + 0.1 * w
    return (w - 0.02 * step).astype(jnp.bfloat16), m, v


def reference(g_w_gate, g_w_up, g_w_down, w_gate, w_up, w_down, m_w_gate, m_w_up, m_w_down, v_w_gate, v_w_up, v_w_down):
    def total(terms):
        return lax.scan(lambda so_far, term: (so_far + term.astype(jnp.float32), None), jnp.zeros(terms.shape[1:], jnp.float32), terms)[0]

    gradients = [total(terms).astype(jnp.bfloat16).astype(jnp.float32) for terms in (g_w_gate, g_w_up, g_w_down)]
    new = [
        adamw(w.astype(jnp.float32), m, v, g)
        for w, m, v, g in zip((w_gate, w_up, w_down), (m_w_gate, m_w_up, m_w_down), (v_w_gate, v_w_up, v_w_down), gradients, strict=True)
    ]
    return tuple(one[which] for which in range(3) for one in new)
```

```python
import math

import jax
import jax.numpy as jnp
from jax import lax
from jax.experimental import pallas as pl
from jax.experimental.pallas import tpu as pltpu
from jax.sharding import PartitionSpec as P

BF, F32 = jnp.bfloat16, jnp.float32
MESH = pl.DeviceIdType.MESH
NX, NY, NZ = 4, 4, 8
LAYERS = 2
UP_ROWS, UP_COLS = 56, 2304
DOWN_ROWS, DOWN_COLS = 144, 896
CUT = 256
SIDE = NZ * CUT
WIDE = UP_COLS + CUT
OWN_UP, OWN_DOWN = 7, 18
TILE_UP, TILE_DOWN = 8, 24


class Place:
    def __init__(self):
        me = lax.axis_index("dp")
        self.me = me
        self.x, self.y, self.z = lax.div(me, NY * NZ), lax.rem(lax.div(me, NZ), NY), lax.rem(me, NZ)

    def at_x(self, by):
        return (lax.rem(self.x + by + NX, NX) * NY + self.y) * NZ + self.z

    def at_y(self, by):
        return (self.x * NY + lax.rem(self.y + by + NY, NY)) * NZ + self.z

    def at_z(self, by):
        return (self.x * NY + self.y) * NZ + lax.rem(self.z + by + NZ, NZ)


def greet(place):
    barrier = pltpu.get_barrier_semaphore()
    peers = [place.at_x(1), place.at_x(-1)] + [place.at_y(j) for j in range(1, NY)] + [place.at_z(j) for j in range(1, NZ)]
    for peer in peers:
        pl.semaphore_signal(barrier, inc=1, device_id={"dp": peer}, device_id_type=MESH)
    pl.semaphore_wait(barrier, len(peers))


class Plan:
    def __init__(self):
        self.steps, self.started = [], []

    def add(self, when, step):
        self.steps.append((when, len(self.steps), step))

    def send(self, copy):
        copy.start()
        self.started.append(copy)

    def run(self):
        for _, _, step in sorted(self.steps, key=lambda s: s[:2]):
            step()
        for copy in self.started:
            copy.wait_send()


def remote(src, dst, send_sem, recv_sem, dev):
    return pltpu.make_async_remote_copy(src_ref=src, dst_ref=dst, send_sem=send_sem, recv_sem=recv_sem, device_id={"dp": dev}, device_id_type=MESH)


def over(shape, block, body):
    *lead, rows, _ = shape
    each = rows // block

    def one(i, _):
        row, rest, index = lax.rem(i, each), lax.div(i, each), []
        for size in reversed(lead):
            index.insert(0, lax.rem(rest, size))
            rest = lax.div(rest, size)
        body((*index, pl.ds(pl.multiple_of(row * block, block), block)))
        return 0

    lax.fori_loop(0, math.prod(lead) * each, one, 0)


def add_to(dst, parts, block):
    def body(index):
        total = parts[0][(*index, slice(None))].astype(F32)
        for part in parts[1:]:
            total = total + part[(*index, slice(None))].astype(F32)
        dst[(*index, slice(None))] = total.astype(dst.dtype)

    over(dst.shape, block, body)


class Ring:
    def __init__(self, plan, n, pos, peer, pieces, start, slot, send_sem, recv_sem, finish):
        self.plan, self.n, self.pos, self.peer, self.pieces = plan, n, pos, peer, pieces
        self.send_sem, self.recv_sem = send_sem, recv_sem
        plan.add(start, self.first)
        for m in range(n - 1):
            due = start + (m + 1) * slot + 2.5
            if m + 2 <= n - 2:
                plan.add(due, lambda m=m: self.forward(m))
        last = start + (n - 1) * slot + 2.5
        plan.add(last, lambda: self.arrive(n - 3))
        plan.add(last, lambda: self.arrive(n - 2))
        plan.add(last, finish)
        self.end = last

    def what(self, way, m):
        k = self.n // 2 - (m + 1) // 2
        layer = m % 2 if way == 0 else 1 - m % 2
        return layer, lax.rem(self.pos + (k if way == 0 else -k) + self.n, self.n)

    def copy(self, way, m, p, source):
        piece = self.pieces[p]
        return remote(source, piece["recv"](way, m), self.send_sem.at[way, m, p], self.recv_sem.at[way, m, p], self.peer(1 if way == 0 else -1))

    def first(self):
        for m in (0, 1):
            for way in (0, 1):
                for p, piece in enumerate(self.pieces):
                    self.plan.send(self.copy(way, m, p, piece["raw"](*self.what(way, m))))

    def arrive(self, m):
        for way in (0, 1):
            for p, piece in enumerate(self.pieces):
                self.copy(way, m, p, piece["recv"](way, m)).wait_recv()

    def forward(self, m):
        for way in (0, 1):
            layer, chunk = self.what(way, m + 2)
            for p, piece in enumerate(self.pieces):
                self.copy(way, m, p, piece["recv"](way, m)).wait_recv()
                own = piece["own"](way, m + 2, layer, chunk)
                add_to(own, [own, piece["recv"](way, m)], piece["block"])
                self.plan.send(self.copy(way, m + 2, p, own))

    def parts(self, p, layer):
        piece, n = self.pieces[p], self.n
        right, left = (n - 2, n - 3) if layer == 0 else (n - 3, n - 2)
        return [piece["mine"](layer), piece["recv"](0, right), piece["recv"](1, left)]


def scatter_kernel(gate, up, down, g0, g1, g2, *scratch):
    (a0_own, a0_recv, b0_recv, t0, c0_recv, f0, a1_own, a1_recv, b1_recv, t1, c1_recv, f1, a2_own, a2_recv, b2_recv, d2_recv, t2, f2) = scratch[:18]
    (local, sa0, ra0, sb0, rb0, sc0, rc0, sa1, ra1, sb1, rb1, sc1, rc1, sa2, ra2, sb2, rb2, sd2, rd2, se2, re2) = scratch[18:]
    place = Place()
    x, y, z = place.x, place.y, place.z
    plan = Plan()
    loads = {}

    def load(name, copies):
        loads[name] = copies
        for copy in copies:
            copy.start()

    def ready(name):
        for copy in loads.pop(name):
            copy.wait()

    def slot(n, way, m):
        return 2 + way * (n - 3) + m - 2

    pieces_a0 = [dict(
        raw=lambda l, c: down.at[l, c],
        own=lambda way, m, l, c: a0_own.at[slot(NX, way, m)],
        mine=lambda l: a0_own.at[l],
        recv=lambda way, m: a0_recv.at[way, m],
        block=16,
    )]
    pieces_a1 = [
        dict(
            raw=lambda l, c: up.at[l, :, c],
            own=lambda way, m, l, c: a1_own.at[slot(NY, way, m), :, :, pl.ds(0, UP_COLS)],
            mine=lambda l: a1_own.at[l, :, :, pl.ds(0, UP_COLS)],
            recv=lambda way, m: a1_recv.at[way, m, :, :, pl.ds(0, UP_COLS)],
            block=8,
        ),
        dict(
            raw=lambda l, c: gate.at[l, :, c, :, pl.ds(SIDE, CUT)],
            own=lambda way, m, l, c: a1_own.at[slot(NY, way, m), :, :, pl.ds(UP_COLS, CUT)],
            mine=lambda l: a1_own.at[l, :, :, pl.ds(UP_COLS, CUT)],
            recv=lambda way, m: a1_recv.at[way, m, :, :, pl.ds(UP_COLS, CUT)],
            block=56,
        ),
    ]
    pieces_a2 = [dict(
        raw=lambda l, c: gate.at[l, :, :, :, pl.ds(pl.multiple_of(c * CUT, CUT), CUT)],
        own=lambda way, m, l, c: a2_own.at[slot(NZ, way, m)],
        mine=lambda l: a2_own.at[l],
        recv=lambda way, m: a2_recv.at[way, m],
        block=56,
    )]

    def fetch(tag, ring, first_sem, messages):
        copies, sem = [], first_sem
        for m in messages:
            for way in (0, 1):
                for piece in ring.pieces:
                    if m is None:
                        src, dst = piece["raw"](way, ring.pos), piece["mine"](way)
                    else:
                        layer, chunk = ring.what(way, m)
                        src, dst = piece["raw"](layer, chunk), piece["own"](way, m, layer, chunk)
                    copies.append(pltpu.make_async_copy(src, dst, local.at[sem]))
                    sem += 1
        load(tag, copies)
        return sem

    def finish_a0():
        ready("mine0")
        for l in range(LAYERS):
            add_to(ring_a0.pieces[0]["mine"](l), ring_a0.parts(0, l), 16)

    def finish_b0():
        for l in range(LAYERS):
            own, right, left = ring_b0.parts(0, l)
            add_to(f0.at[pl.ds(0, DOWN_ROWS)], [own, right, left], 16)
            for c in range(NZ):
                t0[c, l] = f0[pl.ds(c * OWN_DOWN, TILE_DOWN), :].astype(BF)

    def finish_c0():
        for l in range(LAYERS):
            add_to(g0.at[l], ring_c0.parts(0, l), TILE_DOWN)

    ring_a0 = Ring(plan, NX, x, place.at_x, pieces_a0, 0.0, 22.1, sa0, ra0, finish_a0)
    ring_b0 = Ring(plan, NY, y, place.at_y, [dict(
        raw=lambda l, c: a0_own.at[l, c],
        own=lambda way, m, l, c: a0_own.at[l, c],
        mine=lambda l: a0_own.at[l, y],
        recv=lambda way, m: b0_recv.at[way, m],
        block=16,
    )], ring_a0.end + 0.1, 5.6, sb0, rb0, finish_b0)
    ring_c0 = Ring(plan, NZ, z, place.at_z, [dict(
        raw=lambda l, c: t0.at[c, l],
        own=lambda way, m, l, c: t0.at[c, l],
        mine=lambda l: t0.at[z, l],
        recv=lambda way, m: c0_recv.at[way, m],
        block=TILE_DOWN,
    )], ring_b0.end + 0.1, 1.7, sc0, rc0, finish_c0)

    def finish_a1():
        ready("mine1")
        for l in range(LAYERS):
            for p in (0, 1):
                add_to(ring_a1.pieces[p]["mine"](l), ring_a1.parts(p, l), ring_a1.pieces[p]["block"])

    def finish_b1():
        for l in range(LAYERS):
            own, right, left = ring_b1.parts(0, l)
            add_to(f1.at[pl.ds(0, UP_ROWS)], [own, right, left], 8)
            for c in range(NZ):
                t1[c, l] = f1[pl.ds(c * OWN_UP, TILE_UP), :].astype(BF)

    def finish_c1():
        for l in range(LAYERS):
            add_to(g1.at[l], ring_c1.parts(0, l), TILE_UP)

    ring_a1 = Ring(plan, NY, y, place.at_y, pieces_a1, 0.01, 24.6, sa1, ra1, finish_a1)
    ring_b1 = Ring(plan, NX, x, place.at_x, [dict(
        raw=lambda l, c: a1_own.at[l, c],
        own=lambda way, m, l, c: a1_own.at[l, c],
        mine=lambda l: a1_own.at[l, x],
        recv=lambda way, m: b1_recv.at[way, m],
        block=8,
    )], ring_a1.end + 0.1, 6.2, sb1, rb1, finish_b1)
    ring_c1 = Ring(plan, NZ, z, place.at_z, [dict(
        raw=lambda l, c: t1.at[c, l],
        own=lambda way, m, l, c: t1.at[c, l],
        mine=lambda l: t1.at[z, l],
        recv=lambda way, m: c1_recv.at[way, m],
        block=TILE_UP,
    )], ring_b1.end + 0.1, 1.7, sc1, rc1, finish_c1)

    def finish_a2():
        ready("mine2")
        for l in range(LAYERS):
            add_to(ring_a2.pieces[0]["mine"](l), ring_a2.parts(0, l), 56)

    def finish_b2():
        for l in range(LAYERS):
            add_to(ring_b2.pieces[0]["mine"](l), ring_b2.parts(0, l), 56)
        for j in range(1, NY):
            plan.send(across(j))

    def across(j):
        to = lax.rem(y + j, NY)
        return remote(a2_own.at[pl.ds(0, LAYERS), x, to], d2_recv.at[j - 1], sd2.at[j - 1], rd2.at[j - 1], place.at_y(j))

    def finish_d2():
        for j in range(1, NY):
            across(j).wait_recv()
        for l in range(LAYERS):
            add_to(f2.at[pl.ds(0, UP_ROWS)], [a2_own.at[l, x, y]] + [d2_recv.at[j, l] for j in range(NY - 1)], 56)
            for c in range(NZ):
                t2[c, l] = f2[pl.ds(c * OWN_UP, TILE_UP), :].astype(BF)
        for j in range(1, NZ):
            plan.send(turn(j))
        g2[z] = t2[z]

    def turn(j):
        return remote(t2.at[lax.rem(z + j, NZ)], g2.at[z], se2.at[j - 1], re2.at[j - 1], place.at_z(j))

    def finish_e2():
        for j in range(1, NZ):
            turn(j).wait_recv()

    ring_a2 = Ring(plan, NZ, z, place.at_z, pieces_a2, 0.02, 9.85, sa2, ra2, finish_a2)
    ring_b2 = Ring(plan, NX, x, place.at_x, [dict(
        raw=lambda l, c: a2_own.at[l, c],
        own=lambda way, m, l, c: a2_own.at[l, c],
        mine=lambda l: a2_own.at[l, x],
        recv=lambda way, m: b2_recv.at[way, m],
        block=56,
    )], ring_a2.end + 0.1, 4.0, sb2, rb2, finish_b2)
    plan.add(ring_b2.end + 6.0, finish_d2)
    plan.add(max(ring_b2.end + 12.0, ring_c0.end, ring_c1.end) + 1.0, finish_e2)

    def begin():
        f0[pl.ds(DOWN_ROWS, 8), :] = jnp.zeros((8, DOWN_COLS), F32)
        f1[pl.ds(UP_ROWS, 8), :] = jnp.zeros((8, WIDE), F32)
        f2[pl.ds(UP_ROWS, 8), :] = jnp.zeros((8, CUT), F32)
        sem = 0
        for m in range(2, NZ - 1):
            sem = fetch(f"a2_{m}", ring_a2, sem, [m])
            if m == 3:
                sem = fetch("a0", ring_a0, sem, [2])
                sem = fetch("a1", ring_a1, sem, [2])
        sem = fetch("mine2", ring_a2, sem, [None])
        sem = fetch("mine0", ring_a0, sem, [None])
        sem = fetch("mine1", ring_a1, sem, [None])

    plan.add(0.5, begin)
    plan.add(1.0, lambda: ready("a0"))
    plan.add(1.0, lambda: ready("a1"))
    for m in range(2, NZ - 1):
        plan.add(1.0, lambda m=m: ready(f"a2_{m}"))

    greet(place)
    plan.run()


def adamw(w, m, v, g):
    m = 0.9 * m + 0.1 * g
    v = 0.95 * v + 0.05 * g * g
    step = m * lax.rsqrt(v + 1e-8) + 0.1 * w
    return w - 0.02 * step, m, v


def step_kernel(g0, g1, g2, w_gate, w_up, w_down, m_gate, m_up, m_down, v_gate, v_up, v_down,
                n_m_gate, n_m_up, n_m_down, n_v_gate, n_v_up, n_v_down, n0, n1, n2,
                old_gate, old_up, old_down, wide, tall, short, sems):
    place = Place()
    z, slab = place.z, place.x * NY + place.y
    tile = slab * 7 + lax.div(z * OWN_UP, 8)
    copies = []
    for i, (w, old) in enumerate(((w_gate, old_gate), (w_up, old_up))):
        copies.append(pltpu.make_async_copy(w.at[:, tile], old.at[:, 0], sems.at[2 * i]))
        copies.append(pltpu.make_async_copy(w.at[:, tile + 1 - lax.div(z, NZ - 1)], old.at[:, 1], sems.at[2 * i + 1]))
    copies.append(pltpu.make_async_copy(w_down.at[:, pl.ds(slab * 18 + lax.div(z * OWN_DOWN, 8), 3)], old_down, sems.at[4]))
    for copy in copies:
        copy.start()
    for copy in copies:
        copy.wait()
    off = lax.rem(z * OWN_UP, 8)
    short[pl.ds(OWN_UP, 1), :] = jnp.zeros((1, UP_COLS), F32)
    for l in range(LAYERS):
        for old, m, v, n_m, n_v, which in ((old_gate, m_gate, v_gate, n_m_gate, n_v_gate, 0), (old_up, m_up, v_up, n_m_up, n_v_up, 1)):
            for t in range(2):
                wide[pl.ds(t * 8, 8), :] = old[l, t].astype(F32)
            w = pltpu.roll(wide[...], lax.rem(16 - off, 16), 0)[:OWN_UP]
            if which == 0:
                g = jnp.concatenate([g2[s, l] for s in range(NZ)] + [g1[l, :, pl.ds(UP_COLS, CUT)]], axis=1)
            else:
                g = g1[l, :, pl.ds(0, UP_COLS)]
            w, new_m, new_v = adamw(w, m[l], v[l], g.astype(F32)[:OWN_UP])
            n_m[l] = new_m
            n_v[l] = new_v
            short[pl.ds(0, OWN_UP), :] = w
            out = short[...].astype(BF)
            if which == 0:
                for s in range(NZ):
                    n2[s, l] = out[:, s * CUT : (s + 1) * CUT]
                n1[l, :, pl.ds(UP_COLS, CUT)] = out[:, SIDE:]
            else:
                n1[l, :, pl.ds(0, UP_COLS)] = out
    off = lax.rem(z * OWN_DOWN, 8)
    for l in range(LAYERS):
        for t in range(3):
            tall[pl.ds(t * 8, 8), :] = old_down[l, t].astype(F32)
        w = pltpu.roll(tall[pl.ds(0, 24), :], lax.rem(24 - off, 24), 0)[:OWN_DOWN]
        w, new_m, new_v = adamw(w, m_down[l], v_down[l], g0[l].astype(F32)[:OWN_DOWN])
        n_m_down[l] = new_m
        n_v_down[l] = new_v
        tall[pl.ds(0, OWN_DOWN), :] = w
        n0[l] = tall[...].astype(BF)


class Spread:
    def __init__(self, plan, n, pos, peer, pieces, start, slot, send_sem, recv_sem, finish, own=None):
        self.plan, self.n, self.pos, self.peer, self.pieces, self.own = plan, n, pos, peer, pieces, own
        self.send_sem, self.recv_sem = send_sem, recv_sem
        plan.add(start, self.first)
        for m in range(n - 1):
            plan.add(start + (m + 1) * slot + 2.5, lambda m=m: self.forward(m))
        self.end = start + (n - 1) * slot + 2.5
        plan.add(self.end, finish)

    def copy(self, way, m, p, first=False):
        k = m // 2
        layer = m % 2 if way == 0 else 1 - m % 2
        chunk = lax.rem(self.pos + (-k if way == 0 else k) + self.n, self.n)
        ref = self.pieces[p](layer, chunk)
        source = self.own[p](layer) if first and self.own else ref
        return remote(source, ref, self.send_sem.at[way, m, p], self.recv_sem.at[way, m, p], self.peer(1 if way == 0 else -1))

    def first(self):
        for m in (0, 1):
            for way in (0, 1):
                for p in range(len(self.pieces)):
                    self.plan.send(self.copy(way, m, p, True))

    def forward(self, m):
        for way in (0, 1):
            for p in range(len(self.pieces)):
                self.copy(way, m, p).wait_recv()
                if m + 2 <= self.n - 2:
                    self.plan.send(self.copy(way, m + 2, p))


def gather_kernel(n0, n1, n2, gate, up, down, z0, z1, d2, f0, f1, f2, sz0, rz0, sy0, ry0, sx0, rx0, sz1, rz1, sx1, rx1, sy1, ry1, se2, re2, sd2, rd2, sx2, rx2, sz2, rz2):
    place = Place()
    x, y, z = place.x, place.y, place.z
    plan = Plan()
    mine = pl.ds(pl.multiple_of(z * CUT, CUT), CUT)

    def build0():
        z0[z] = n0[...]
        for l in range(LAYERS):
            for c in range(NZ):
                f0[pl.ds(c * OWN_DOWN, OWN_DOWN), :] = z0[c, l].astype(F32)[:OWN_DOWN]
            add_to(down.at[l, x, y], [f0], 16)

    spread_z0 = Spread(plan, NZ, z, place.at_z, [lambda l, c: z0.at[c, l]], 0.01, 1.7, sz0, rz0, build0, [lambda l: n0.at[l]])
    spread_y0 = Spread(plan, NY, y, place.at_y, [lambda l, c: down.at[l, x, c]], spread_z0.end + 0.1, 5.6, sy0, ry0, lambda: None)
    Spread(plan, NX, x, place.at_x, [lambda l, c: down.at[l, c]], spread_y0.end + 0.1, 22.1, sx0, rx0, lambda: None)

    def build1():
        z1[z] = n1[...]
        for l in range(LAYERS):
            for c in range(NZ):
                f1[pl.ds(c * OWN_UP, OWN_UP), :] = z1[c, l].astype(F32)[:OWN_UP]
            add_to(up.at[l, x, y], [f1.at[:, pl.ds(0, UP_COLS)]], 8)
            add_to(gate.at[l, x, y, :, pl.ds(SIDE, CUT)], [f1.at[:, pl.ds(UP_COLS, CUT)]], 8)

    spread_z1 = Spread(plan, NZ, z, place.at_z, [lambda l, c: z1.at[c, l]], 0.02, 1.7, sz1, rz1, build1, [lambda l: n1.at[l]])
    spread_x1 = Spread(plan, NX, x, place.at_x, [lambda l, c: up.at[l, c, y], lambda l, c: gate.at[l, c, y, :, pl.ds(SIDE, CUT)]], spread_z1.end + 0.1, 6.2, sx1, rx1, lambda: None)
    Spread(plan, NY, y, place.at_y, [lambda l, c: up.at[l, :, c], lambda l, c: gate.at[l, :, c, :, pl.ds(SIDE, CUT)]], spread_x1.end + 0.1, 24.6, sy1, ry1, lambda: None)

    def turn(j):
        return remote(n2.at[lax.rem(z + j, NZ)], d2.at[z], se2.at[j - 1], re2.at[j - 1], place.at_z(j))

    def begin2():
        for j in range(1, NZ):
            plan.send(turn(j))
        d2[z] = n2[z]

    def across(j):
        here = gate.at[:, x, y, :, mine]
        return remote(here, here, sd2.at[j - 1], rd2.at[j - 1], place.at_y(j))

    def build2():
        for j in range(1, NZ):
            turn(j).wait_recv()
        for l in range(LAYERS):
            for c in range(NZ):
                f2[pl.ds(c * OWN_UP, OWN_UP), :] = d2[c, l].astype(F32)[:OWN_UP]
            add_to(gate.at[l, x, y, :, mine], [f2], 56)
        for j in range(1, NY):
            plan.send(across(j))

    def across_done():
        for j in range(1, NY):
            across(j).wait_recv()

    plan.add(0.0, begin2)
    plan.add(6.0, build2)
    plan.add(12.0, across_done)
    spread_x2 = Spread(plan, NX, x, place.at_x, [lambda l, c: gate.at[l, c, :, :, mine]], 12.1, 4.0, sx2, rx2, lambda: None)
    Spread(plan, NZ, z, place.at_z, [lambda l, c: gate.at[l, :, :, :, pl.ds(pl.multiple_of(c * CUT, CUT), CUT)]], spread_x2.end + 0.1, 9.85, sz2, rz2, lambda: None)

    greet(place)
    plan.run()


def out_kernel(*refs):
    sources, results, sems = refs[:3], refs[3:6], refs[6]
    copies = [pltpu.make_async_copy(a.at[l, i], b.at[l, i], sems.at[w, l, i]) for w, (a, b) in enumerate(zip(sources, results)) for l in range(LAYERS) for i in range(NX)]
    for copy in copies:
        copy.start()
    for copy in copies:
        copy.wait()


def ring_sems(n, pieces=1):
    return [pltpu.SemaphoreType.DMA((2, n - 1, pieces))] * 2


def solution(mesh):
    anywhere, vmem = pl.BlockSpec(memory_space=pltpu.HBM), pl.BlockSpec(memory_space=pltpu.VMEM)

    def body(*arrays):
        gate, up, down = (t.reshape(LAYERS, NX, NY, rows, cols) for t, rows, cols in zip(arrays[:3], (UP_ROWS, UP_ROWS, DOWN_ROWS), (UP_COLS, UP_COLS, DOWN_COLS)))
        g0, g1, g2 = pl.pallas_call(
            scatter_kernel,
            name="scatter",
            out_shape=[jax.ShapeDtypeStruct((LAYERS, TILE_DOWN, DOWN_COLS), BF), jax.ShapeDtypeStruct((LAYERS, TILE_UP, WIDE), BF), jax.ShapeDtypeStruct((NZ, LAYERS, TILE_UP, CUT), BF)],
            in_specs=[anywhere] * 3,
            out_specs=[vmem] * 3,
            scratch_shapes=[
                pltpu.VMEM((2 + 2 * (NX - 3), NY, DOWN_ROWS, DOWN_COLS), BF),
                pltpu.VMEM((2, NX - 1, NY, DOWN_ROWS, DOWN_COLS), BF),
                pltpu.VMEM((2, NY - 1, DOWN_ROWS, DOWN_COLS), BF),
                pltpu.VMEM((NZ, LAYERS, TILE_DOWN, DOWN_COLS), BF),
                pltpu.VMEM((2, NZ - 1, TILE_DOWN, DOWN_COLS), BF),
                pltpu.VMEM((DOWN_ROWS + 8, DOWN_COLS), F32),
                pltpu.VMEM((2 + 2 * (NY - 3), NX, UP_ROWS, WIDE), BF),
                pltpu.VMEM((2, NY - 1, NX, UP_ROWS, WIDE), BF),
                pltpu.VMEM((2, NX - 1, UP_ROWS, WIDE), BF),
                pltpu.VMEM((NZ, LAYERS, TILE_UP, WIDE), BF),
                pltpu.VMEM((2, NZ - 1, TILE_UP, WIDE), BF),
                pltpu.VMEM((UP_ROWS + 8, WIDE), F32),
                pltpu.VMEM((2 + 2 * (NZ - 3), NX, NY, UP_ROWS, CUT), BF),
                pltpu.VMEM((2, NZ - 1, NX, NY, UP_ROWS, CUT), BF),
                pltpu.VMEM((2, NX - 1, NY, UP_ROWS, CUT), BF),
                pltpu.VMEM((NY - 1, LAYERS, UP_ROWS, CUT), BF),
                pltpu.VMEM((NZ, LAYERS, TILE_UP, CUT), BF),
                pltpu.VMEM((UP_ROWS + 8, CUT), F32),
                pltpu.SemaphoreType.DMA((2 * (NZ - 3) + 2 + 4 + 8,)),
                *ring_sems(NX), *ring_sems(NY), *ring_sems(NZ),
                *ring_sems(NY, 2), *ring_sems(NX), *ring_sems(NZ),
                *ring_sems(NZ), *ring_sems(NX),
                *[pltpu.SemaphoreType.DMA((NY - 1,))] * 2,
                *[pltpu.SemaphoreType.DMA((NZ - 1,))] * 2,
            ],
            compiler_params=pltpu.CompilerParams(collective_id=0, has_side_effects=True, vmem_limit_bytes=60 * 2**20),
        )(gate, up, down)

        w_gate, w_up, w_down = (w.reshape(LAYERS, -1, 8, w.shape[-1]) for w in arrays[3:6])
        moments = arrays[6:12]
        *new, n0, n1, n2 = pl.pallas_call(
            step_kernel,
            name="step",
            out_shape=[jax.ShapeDtypeStruct(a.shape, F32) for a in moments] + [jax.ShapeDtypeStruct(a.shape, BF) for a in (g0, g1, g2)],
            in_specs=[vmem] * 3 + [anywhere] * 3 + [vmem] * 6,
            out_specs=[vmem] * 9,
            scratch_shapes=[
                pltpu.VMEM((LAYERS, 2, 8, UP_COLS), BF),
                pltpu.VMEM((LAYERS, 2, 8, UP_COLS), BF),
                pltpu.VMEM((LAYERS, 3, 8, DOWN_COLS), BF),
                pltpu.VMEM((16, UP_COLS), F32),
                pltpu.VMEM((TILE_DOWN, DOWN_COLS), F32),
                pltpu.VMEM((8, UP_COLS), F32),
                pltpu.SemaphoreType.DMA((5,)),
            ],
            compiler_params=pltpu.CompilerParams(vmem_limit_bytes=20 * 2**20),
        )(g0, g1, g2, w_gate, w_up, w_down, *moments)

        whole = pl.pallas_call(
            gather_kernel,
            name="gather",
            out_shape=[pltpu.VMEM(a.shape, BF) for a in (gate, up, down)],
            in_specs=[vmem] * 3,
            out_specs=[vmem] * 3,
            scratch_shapes=[
                pltpu.VMEM((NZ, LAYERS, TILE_DOWN, DOWN_COLS), BF),
                pltpu.VMEM((NZ, LAYERS, TILE_UP, WIDE), BF),
                pltpu.VMEM((NZ, LAYERS, TILE_UP, CUT), BF),
                pltpu.VMEM((DOWN_ROWS, DOWN_COLS), F32),
                pltpu.VMEM((UP_ROWS, WIDE), F32),
                pltpu.VMEM((UP_ROWS, CUT), F32),
                *ring_sems(NZ), *ring_sems(NY), *ring_sems(NX),
                *ring_sems(NZ), *ring_sems(NX, 2), *ring_sems(NY, 2),
                *[pltpu.SemaphoreType.DMA((NZ - 1,))] * 2,
                *[pltpu.SemaphoreType.DMA((NY - 1,))] * 2,
                *ring_sems(NX), *ring_sems(NZ),
            ],
            compiler_params=pltpu.CompilerParams(collective_id=1, has_side_effects=True, vmem_limit_bytes=16 * 2**20),
        )(n0, n1, n2)
        whole = pl.pallas_call(
            out_kernel,
            name="out",
            out_shape=[jax.ShapeDtypeStruct(a.shape, BF) for a in (gate, up, down)],
            in_specs=[vmem] * 3,
            out_specs=[anywhere] * 3,
            scratch_shapes=[pltpu.SemaphoreType.DMA((3, LAYERS, NX))],
            compiler_params=pltpu.CompilerParams(vmem_limit_bytes=2 * 2**20),
        )(*whole)
        whole = [w.reshape(LAYERS, -1, w.shape[-1]) for w in whole]
        return (*whole, *new)

    all_of, cut = P(None, None, None), P(None, "dp", None)
    return jax.shard_map(
        body,
        mesh=mesh,
        in_specs=(P(("rep", "dp"), None, None, None),) * 3 + (all_of,) * 3 + (cut,) * 6,
        out_specs=(P("rep", None, None),) * 3 + (P("rep", "dp", None),) * 6,
        check_vma=False,
    )
```
